32 devices in a mesh: band: 8 (over z, x), dir: 4 (over y, core).
Axes of the slice: x: 2, y: 2, z: 4, core: 2. Of those that a mesh axis runs over, the one named last changes fastest.
Arguments:
- visibilities: bfloat16 [16, 32, 2, 256, 256], P('band', 'dir'), as said below
- sky_model: bfloat16 [16, 32, 2, 256, 256], P('band', 'dir')
- rfi_flags: int32 [16, 8, 8], P('band'), may hold values from 0 to 1, as said below
- destination: int32 [16], P('band'), may hold values from 0 to 15, as said below
Outputs:
- delivered: float32 [16, 32, 2, 256], P('band', 'dir')
- coefficients: float32 [9, 32, 2, 256], P(None, 'dir')
- norm_values: float32 [2, 2], replicated
The draws below stay inside these ranges and needn't reach their ends.
Inputs may be any that keep to these rules, and one draw needn't show every extreme that they name: `rfi_flags`: 1 marks a flagged baseline block; the share of flagged blocks tends to fall with the subband index. destination holds every row of 0 to 15 once. With the rows split into 8 aligned blocks of 2 rows, one row of block i goes to a row of block i + 1 and the other to a row of block i + 4, modulo 16 // 2. `visibilities`: visibilities follow the model under unknown station gains, with noise.
All inputs are finite; a program needn't handle non-finite values.
Results may differ from the reference program's by a relative error of at most 0.0003.
Values sent between devices are 32-bit elements; how exact they have to be, the bound alone decides.
A program may use at most 128 MiB of HBM per device.

```python
import jax
import jax.numpy as jnp
from jax import lax

STATIONS = 256
DIRECTIONS = 32
BLOCK = 32
DEGREE = 8
SWEEPS = 4
ITERS = 2
SB_DEV = 2
SUBBANDS = 16


def band_pair(key, band_row):
    band_key = jax.random.fold_in(jax.random.fold_in(key, 11), band_row)
    model_key, noise_key, rough_key = jax.random.split(band_key, 3)
    shared = jax.random.normal(jax.random.fold_in(key, 23), (4, DIRECTIONS, STATIONS), jnp.float32)
    rough = jax.random.normal(rough_key, (2, DIRECTIONS, STATIONS), jnp.float32)
    abscissa = (2.0 * band_row.astype(jnp.float32) + 1.0) / SUBBANDS - 1.0
    sky_values = jax.random.normal(model_key, (DIRECTIONS, 2, STATIONS, STATIONS), jnp.float32)
    noise_level = 0.5
    amp_spread = 0.25
    amplitude = 1.0 + amp_spread * shared[0] + 0.15 * abscissa * shared[1] + 0.1 * rough[0]
    phase = 0.8 * shared[2] + 0.5 * abscissa * shared[3] + 0.2 * rough[1]
    gain_re = amplitude * jnp.cos(phase)
    gain_im = amplitude * jnp.sin(phase)
    model_re = sky_values[:, 0]
    model_im = sky_values[:, 1]
    twist_re = model_re * gain_re[:, None, :] + model_im * gain_im[:, None, :]
    twist_im = model_im * gain_re[:, None, :] - model_re * gain_im[:, None, :]
    noise = jax.random.normal(noise_key, (2, DIRECTIONS, STATIONS, STATIONS), jnp.float32)
    data_re = gain_re[:, :, None] * twist_re - gain_im[:, :, None] * twist_im + noise_level * noise[0]
    data_im = gain_re[:, :, None] * twist_im + gain_im[:, :, None] * twist_re + noise_level * noise[1]
    return (sky_values.astype(jnp.bfloat16), jnp.stack([data_re, data_im], axis=1).astype(jnp.bfloat16))


def draw_sky_model(key, part):

    def one_band(band_row):
        return band_pair(key, band_row)[0]
    return lax.map(one_band, jnp.arange(SUBBANDS))


def draw_visibilities(key, part):

    def one_band(band_row):
        return band_pair(key, band_row)[1]
    return lax.map(one_band, jnp.arange(SUBBANDS))


def draw_rfi_flags(key, part):
    band_rows = jnp.arange(SUBBANDS)
    threshold = 750 - 600 * band_rows // max(SUBBANDS - 1, 1)
    blocks = STATIONS // BLOCK
    random_ints = jax.random.randint(jax.random.fold_in(key, 5), (SUBBANDS, blocks, blocks), 0, 1000)
    return (random_ints < threshold[:, None, None]).astype(jnp.int32)


def draw_destination(key, part):
    block_count = SUBBANDS // SB_DEV
    half_count = block_count // 2
    base_key = jax.random.fold_in(key, 7)
    send_key, recv_key = jax.random.split(base_key)
    send_perm = jax.vmap(lambda one_key: jax.random.permutation(one_key, SB_DEV))(jax.random.split(send_key, block_count))
    recv_perm = jax.vmap(lambda one_key: jax.random.permutation(one_key, SB_DEV))(jax.random.split(recv_key, block_count))
    block_ids = jnp.arange(block_count)[:, None]
    slot_ids = jnp.arange(SB_DEV)[None, :]
    source_rows = block_ids * SB_DEV + send_perm
    target_block = jnp.where(slot_ids == 0, (block_ids + 1) % block_count, jnp.where(slot_ids == 1, (block_ids + half_count) % block_count, block_ids + 0 * slot_ids))
    target_slot = recv_perm[target_block, slot_ids + 0 * block_ids]
    target_rows = target_block * SB_DEV + target_slot
    result = jnp.zeros((SUBBANDS,), jnp.int32).at[source_rows.reshape(-1)].set(target_rows.reshape(-1).astype(jnp.int32))
    return result.astype(jnp.int32)


def setup_inputs(seed: int = 0) -> dict:
    streams_of = jax.random.split(jax.random.key(seed), 5)
    return {
        "visibilities": draw_visibilities(jax.random.fold_in(streams_of[4], 71), 0),
        "sky_model": draw_sky_model(jax.random.fold_in(streams_of[4], 71), 0),
        "rfi_flags": draw_rfi_flags(jax.random.fold_in(streams_of[4], 71), 0),
        "destination": draw_destination(jax.random.fold_in(streams_of[4], 71), 0),
    }


highest = lax.Precision.HIGHEST
penalty_share = 0.4

def block_weights(rfi_flags):
    blocks = rfi_flags.shape[-1]
    kept_blocks = (1 - rfi_flags).astype(jnp.float32)
    leading = kept_blocks.shape[:-2]
    spread = jnp.broadcast_to(kept_blocks[..., :, None, :, None], leading + (blocks, BLOCK, blocks, BLOCK))
    stations = blocks * BLOCK
    spread = spread.reshape(leading + (stations, stations))
    return spread * (1.0 - jnp.eye(stations, dtype=jnp.float32))

def operators(visibilities, sky_model, rfi_flags):
    baseline = block_weights(rfi_flags)[..., None, :, :]
    data_re = visibilities[..., 0, :, :].astype(jnp.float32)
    data_im = visibilities[..., 1, :, :].astype(jnp.float32)
    model_re = sky_model[..., 0, :, :].astype(jnp.float32)
    model_im = sky_model[..., 1, :, :].astype(jnp.float32)
    oper_re = baseline * (model_re * data_re + model_im * data_im)
    oper_im = baseline * (model_re * data_im - model_im * data_re)
    square = baseline * (model_re * model_re + model_im * model_im)
    return (jnp.stack([oper_re, oper_im], axis=-3), square)

def chebyshev(band_rows, band_total):
    abscissa = (2.0 * band_rows + 1.0) / band_total - 1.0
    cheb_terms = [jnp.ones_like(abscissa), abscissa]
    for degree in range(2, DEGREE + 1):
        cheb_terms.append(2.0 * abscissa * cheb_terms[-1] - cheb_terms[-2])
    return jnp.stack(cheb_terms[:DEGREE + 1], axis=0)

def stefcal(operator, square, gain_now, target, penalty):
    pen_term = penalty[..., None, None, None]
    for sweep_index in range(SWEEPS):
        products = jnp.einsum('...kapq,...kbq->...kabp', operator, gain_now, precision=highest)
        real_part = products[..., 0, 0, :] - products[..., 1, 1, :]
        imag_part = products[..., 0, 1, :] + products[..., 1, 0, :]
        numerator = jnp.stack([real_part, imag_part], axis=-2)
        magnitude = lax.optimization_barrier(jnp.sum(gain_now * gain_now, axis=-2))
        denominator = jnp.einsum('...kpq,...kq->...kp', square, magnitude, precision=highest)
        updated = (numerator + pen_term * target) / (denominator[..., None, :] + pen_term)
        gain_now = 0.5 * (updated + gain_now) if sweep_index % 2 == 1 else updated
    return gain_now

def per_band(band_items):
    vis_band, model_band, flag_band, gain_band, target_band, pen_band = band_items
    operator, square = operators(vis_band, model_band, flag_band)
    return stefcal(operator, square, gain_band, target_band, pen_band)

def reference(visibilities, sky_model, rfi_flags, destination):
    band_total = visibilities.shape[0]
    directions = visibilities.shape[1]
    stations = visibilities.shape[-1]
    blocks = rfi_flags.shape[-1]
    weights = (1.0 + lax.optimization_barrier(jnp.sum(1 - rfi_flags, axis=(1, 2))).astype(jnp.float32)) / (1.0 + blocks * blocks)
    penalty = penalty_share * stations * weights
    cheb_basis = chebyshev(jnp.arange(band_total).astype(jnp.float32), band_total)
    weighted = cheb_basis * weights[None, :]
    gram_matrix = jnp.dot(weighted, cheb_basis.T, precision=highest)
    factor = jnp.linalg.cholesky(gram_matrix)
    normalizer = directions * 2.0 * stations * gram_matrix[0, 0]
    ones_part = jnp.ones((band_total, directions, stations), jnp.float32)
    unit_gains = jnp.stack([ones_part, jnp.zeros_like(ones_part)], axis=2)
    gain_now = unit_gains
    consensus = unit_gains
    dual_var = jnp.zeros_like(unit_gains)
    row_weight = weights[:, None, None, None]
    norm_rows = []
    coefficients = None
    for iteration in range(ITERS):
        gain_now = lax.map(per_band, (visibilities, sky_model, rfi_flags, gain_now, consensus - dual_var, penalty))
        projection = jnp.einsum('cs,skap->ckap', weighted, gain_now + dual_var, precision=highest)
        flat_proj = projection.reshape(projection.shape[0], -1)
        coefficients = jax.scipy.linalg.cho_solve((factor, True), flat_proj).reshape(projection.shape)
        fresh_gains = jnp.einsum('cs,ckap->skap', cheb_basis, coefficients, precision=highest)
        dual_var = dual_var + gain_now - fresh_gains
        primal = jnp.sqrt(jnp.sum(row_weight * (gain_now - fresh_gains) ** 2) / normalizer)
        dual_norm = jnp.sqrt(jnp.sum(row_weight * (fresh_gains - consensus) ** 2) / normalizer)
        norm_rows.append(jnp.stack([primal, dual_norm]))
        consensus = fresh_gains
    delivered = jnp.zeros_like(gain_now).at[destination].set(gain_now)
    return (delivered, coefficients, jnp.stack(norm_rows))
```

```python
import functools

import jax
import jax.numpy as jnp
from jax import lax
from jax.experimental import pallas as pl
from jax.experimental.pallas import tpu as pltpu
from jax.sharding import PartitionSpec as P

BLOCK = 32
DEGREE = 8
SWEEPS = 4
ITERS = 2
TERMS = DEGREE + 1
ROWS = 16
LANES = 128
TILE = 8
PLAN = (("exact", "lead", "both", "held"), ("held", "held", "both", "held"))

penalty_share = 0.4
f32 = jnp.float32
bf16 = jnp.bfloat16
MESH = pl.DeviceIdType.MESH


def row_of(shape, axis=0):
    return lax.broadcasted_iota(jnp.int32, shape, axis)


def spread(value, shape):
    return jnp.broadcast_to(value, shape)


def repeat(count, body, carry):
    if count <= 8:
        for i in range(count):
            carry = body(i, carry)
        return carry
    return lax.fori_loop(0, count, body, carry)


def kernel(
    bands,
    dirs,
    group,
    vis_hbm,
    sky_hbm,
    flags,
    dest,
    delivered,
    coef,
    norms,
    vis,
    sky,
    lead_num,
    lead_den,
    rest_num,
    rest_den,
    turned,
    keep,
    wpen,
    meta,
    gains,
    zall,
    uall,
    held,
    solve_rows,
    cheb_rows,
    solve_tiles,
    cheb_tiles,
    norm_all,
    vis_sem,
    sky_sem,
    meta_send,
    meta_recv,
    gain_send,
    gain_recv,
    norm_send,
    norm_recv,
):
    subs, count, _, stations, _ = vis_hbm.shape
    blocks = flags.shape[-1]
    total = bands * subs
    width = meta.shape[-1]
    chunks = count // group
    pairs = subs * group
    rows = 2 * pairs
    me = lax.axis_index("band")
    my_dir = lax.axis_index("dir")
    tile = (rows, stations)

    def ahead(distance):
        return lax.rem(me + distance, bands)

    def behind(distance):
        return lax.rem(me + bands - distance, bands)

    def load(c, j):
        s, k = j // group, c * group + j % group
        slot = c * pairs + j
        return (
            pltpu.make_async_copy(vis_hbm.at[s, k], vis.at[slot], vis_sem.at[slot]),
            pltpu.make_async_copy(sky_hbm.at[s, k], sky.at[slot], sky_sem.at[slot]),
        )

    for c in range(chunks):
        for j in range(pairs):
            for copy in load(c, j):
                copy.start()

    barrier = pltpu.get_barrier_semaphore()
    for distance in range(1, bands):
        pl.semaphore_signal(
            barrier, inc=1, device_id={"band": ahead(distance)}, device_id_type=MESH
        )
    for distance in range(1, dirs):
        pl.semaphore_signal(
            barrier,
            inc=1,
            device_id={"dir": lax.rem(my_dir + distance, dirs)},
            device_id_type=MESH,
        )

    row = row_of(tile)
    odd = lax.rem(row, 2) == 1
    sub_row = row // (2 * group)

    lane_w = row_of((1, width), 1)
    weight_row = jnp.zeros((1, width), f32)
    penalty = jnp.zeros(tile, f32)
    dest_rows = []
    for s in range(subs):
        kept = (1 - flags[s]).astype(f32)
        weight = (1.0 + jnp.sum(kept, axis=(0, 1), keepdims=True)) / (1.0 + blocks * blocks)
        penalty = jnp.where(sub_row == s, spread(penalty_share * stations * weight, tile), penalty)
        weight_row = jnp.where(lane_w == me * subs + s, weight, weight_row)
        dest_rows.append(jnp.full((1, width), dest[s], jnp.int32).astype(f32))
        lane = row_of((1, stations), 1) // BLOCK
        for i in range(blocks):
            shape = (BLOCK, stations)
            across = jnp.zeros((1, stations), f32)
            for j in range(blocks):
                across = jnp.where(lane == j, kept[j : j + 1, i : i + 1], across)
            apart = row_of(shape) + i * BLOCK != row_of(shape, 1)
            keep[s, i * BLOCK : (i + 1) * BLOCK, :] = jnp.where(
                apart, spread(across, shape), 0.0
            )
    wpen[...] = penalty
    meta[me] = jnp.zeros(meta.shape[1:], f32)
    for s in range(subs):
        meta[me, s : s + 1, :] = dest_rows[s]
    meta[me, subs : subs + 1, :] = weight_row

    def meta_copy(slot, distance):
        return pltpu.make_async_remote_copy(
            src_ref=meta.at[slot],
            dst_ref=meta.at[slot],
            send_sem=meta_send.at[distance],
            recv_sem=meta_recv.at[distance],
            device_id={"band": ahead(distance)},
            device_id_type=MESH,
        )

    def gain_copy(it, c, slot, distance):
        return pltpu.make_async_remote_copy(
            src_ref=gains.at[it, c, slot],
            dst_ref=gains.at[it, c, slot],
            send_sem=gain_send.at[it, c, distance],
            recv_sem=gain_recv.at[it, c, distance],
            device_id={"band": ahead(distance)},
            device_id_type=MESH,
        )

    def norm_copy(slot, distance):
        return pltpu.make_async_remote_copy(
            src_ref=norm_all.at[slot],
            dst_ref=norm_all.at[slot],
            send_sem=norm_send.at[distance],
            recv_sem=norm_recv.at[distance],
            device_id={"dir": lax.rem(my_dir + distance, dirs)},
            device_id_type=MESH,
        )

    square = (stations, stations)
    identity = (row_of(square) == row_of(square, 1)).astype(f32).astype(bf16)
    ones = jnp.where(odd, jnp.zeros(tile, f32), 1.0)

    def swapped(value):
        return jnp.where(odd, pltpu.roll(value, 1, 0), pltpu.roll(value, rows - 1, 0))

    pick_row = row_of((2 * rows, stations))
    pick_pair = lax.rem(pick_row, rows) // 2
    picks = [
        jnp.where(pick_pair == j, jnp.ones(pick_row.shape, f32), 0.0).astype(bf16)
        for j in range(pairs)
    ]

    def left_sides(gain):
        other = swapped(gain)
        sides = []
        for full in (gain, jnp.where(odd, other, -other), gain * gain + other * other):
            lead = full.astype(bf16).astype(f32)
            sides.append(jnp.concatenate([lead, full - lead], axis=0).astype(bf16))
        num, den = [], []
        for j in range(pairs):
            num += [sides[0] * picks[j], sides[1] * picks[j]]
            den.append(sides[2] * picks[j])
        return jnp.concatenate(num, axis=1), jnp.concatenate(den, axis=1)

    def times(left, right):
        out = lax.dot_general(
            left, right, (((1,), (0,)), ((), ())), preferred_element_type=f32
        )
        return out[:rows] + out[rows:]

    def solved(num, den, target):
        pen = wpen[...]
        return (num + pen * target) / (den + pen)

    def build(c, out):
        num = jnp.zeros(tile, f32)
        den = jnp.zeros(tile, f32)

        def turn(j):
            slot = c * pairs + j
            for part, source in enumerate((vis, sky)):
                for i in range(2):
                    turned[j, 2 * part + i] = lax.dot_general(
                        identity,
                        source[slot, i],
                        (((1,), (1,)), ((), ())),
                        preferred_element_type=f32,
                    )

        def fill(j, num, den):
            s = j // group
            sums = [jnp.zeros((TILE, stations), f32) for _ in range(3)]
            for i in range(stations // BLOCK):
                part = slice(i * BLOCK, (i + 1) * BLOCK)
                baseline = keep[s, part, :]
                data_re = turned[j, 0, part, :]
                data_im = turned[j, 1, part, :]
                model_re = baseline * turned[j, 2, part, :]
                model_im = baseline * turned[j, 3, part, :]
                values = (
                    model_re * data_re + model_im * data_im,
                    model_re * data_im - model_im * data_re,
                    model_re * model_re + model_im * model_im,
                )
                for n, full in enumerate(values):
                    for r in range(0, BLOCK, TILE):
                        sums[n] = sums[n] + full[r : r + TILE]
                    lead = full.astype(bf16)
                    rest = (full - lead.astype(f32)).astype(bf16)
                    if n < 2:
                        base = (2 * j + n) * stations + i * BLOCK
                        lead_num[c, base : base + BLOCK, :] = lead
                        rest_num[c, base : base + BLOCK, :] = rest
                    else:
                        base = j * stations + i * BLOCK
                        lead_den[c, base : base + BLOCK, :] = lead
                        rest_den[c, base : base + BLOCK, :] = rest
            re, im, mag = (spread(jnp.sum(x, axis=0, keepdims=True), tile) for x in sums)
            num = jnp.where(row == 2 * j, re, jnp.where(row == 2 * j + 1, im, num))
            den = jnp.where(row // 2 == j, mag, den)
            return num, den

        for j in range(pairs):
            turn(j)
            num, den = fill(j, num, den)
            yield
        out[c] = solved(num, den, ones)

    def sweeps(it, c, gain, out):
        target = ones if it == 0 else zall[c, me] - uall[c, me]
        for index in range(SWEEPS):
            mode = PLAN[it][index]
            if mode == "exact":
                continue
            left_num, left_den = left_sides(gain)
            num = times(left_num, lead_num[c])
            den = times(left_den, lead_den[c])
            if mode == "both":
                low_num = times(left_num, rest_num[c])
                low_den = times(left_den, rest_den[c])
                held[c, 0] = low_num
                held[c, 1] = low_den
                num, den = num + low_num, den + low_den
            yield
            if mode == "held":
                num, den = num + held[c, 0], den + held[c, 1]
            updated = solved(num, den, target)
            gain = 0.5 * (updated + gain) if index % 2 == 1 else updated
        out[c] = gain

    def together(*steps):
        steps = list(steps)
        while steps:
            for step in list(steps):
                try:
                    next(step)
                except StopIteration:
                    steps.remove(step)

    def send(it, c, gain):
        gains[it, c, me] = gain
        for distance in range(1, bands):
            gain_copy(it, c, me, distance).start()

    def arrive(it, c):
        for distance in range(1, bands):
            gain_copy(it, c, behind(distance), distance).wait_recv()

    def solve():
        weights = meta[0, subs : subs + 1, :]
        for i in range(1, bands):
            weights = weights + meta[i, subs : subs + 1, :]
        index = row_of((1, width), 1).astype(f32)
        abscissa = (2.0 * index + 1.0) / total - 1.0
        terms = [jnp.ones_like(abscissa), abscissa]
        for degree in range(2, DEGREE + 1):
            terms.append(2.0 * abscissa * terms[-1] - terms[-2])
        shape = (ROWS, width)
        cheb = jnp.zeros(shape, f32)
        for c in range(TERMS):
            cheb = jnp.where(row_of(shape) == c, spread(terms[c], shape), cheb)
        right = cheb * weights
        gram = jnp.zeros((ROWS, LANES), f32)
        for c in range(TERMS):
            column = jnp.sum(right * terms[c], axis=1, keepdims=True)
            gram = jnp.where(row_of(gram.shape, 1) == c, column, gram)
        for c in range(TERMS):
            pivot = gram[c : c + 1, c : c + 1]
            gram_row = gram[c : c + 1, :] / pivot
            right_row = right[c : c + 1, :] / pivot
            column = gram[:, c : c + 1]
            gram = jnp.where(row_of(gram.shape) == c, gram_row, gram - column * gram_row)
            right = jnp.where(row_of(shape) == c, right_row, right - column * right_row)
        cheb = jnp.where(row_of(shape) == ROWS - 1, spread(weights, shape), cheb)
        for f in range(total):
            solve_rows[f] = spread(right[:, f : f + 1], (ROWS, LANES))
            cheb_rows[f] = spread(cheb[:, f : f + 1], (ROWS, LANES))

        half = (rows, LANES)
        sub = row_of(half) // (2 * group)

        def lay(i, carry):
            for source, tiles, used in (
                (solve_rows, solve_tiles, range(TERMS)),
                (cheb_rows, cheb_tiles, [*range(TERMS), ROWS - 1]),
            ):
                for n, c in enumerate(used):
                    value = spread(source[i * subs, c : c + 1, :], half)
                    for s in range(1, subs):
                        more = spread(source[i * subs + s, c : c + 1, :], half)
                        value = jnp.where(sub == s, more, value)
                    tiles[i, n] = value
            return carry

        repeat(bands, lay, 0)
        return jnp.sum(weights, axis=1, keepdims=True)

    def consensus(it, c, sums):
        parts = [slice(at, at + LANES) for at in range(0, stations, LANES)]
        zero = jnp.zeros((rows, LANES), f32)
        lanes = len(parts)

        def project(i, acc):
            values = []
            for part in parts:
                value = gains[it, c, i, :, part]
                if it > 0:
                    value = value + uall[c, i, :, part]
                values.append(value)
            acc = list(acc)
            for n in range(TERMS):
                scale = solve_tiles[i, n]
                for h in range(lanes):
                    acc[n * lanes + h] = acc[n * lanes + h] + scale * values[h]
            return tuple(acc)

        acc = repeat(bands, project, (zero,) * (TERMS * lanes))
        coefs = []
        for one in acc:
            value = one
            for s in range(1, subs):
                value = value + pltpu.roll(one, s * 2 * group, 0)
            coefs.append(value)
        if it == ITERS - 1:
            for n in range(TERMS):
                for h, part in enumerate(parts):
                    for k in range(group):
                        coef[n, c * group + k, :, part] = coefs[n * lanes + h][2 * k : 2 * k + 2]
        unit = jnp.where(lax.rem(row_of(zero.shape), 2) == 1, zero, 1.0)

        def expand(i, sums):
            primal, dual = sums
            scales = [cheb_tiles[i, n] for n in range(TERMS + 1)]
            for h, part in enumerate(parts):
                fresh = scales[0] * coefs[h]
                for n in range(1, TERMS):
                    fresh = fresh + scales[n] * coefs[n * lanes + h]
                gap = gains[it, c, i, :, part] - fresh
                moved = fresh - (zall[c, i, :, part] if it > 0 else unit)
                primal = primal + scales[TERMS] * (gap * gap)
                dual = dual + scales[TERMS] * (moved * moved)
                if it < ITERS - 1:
                    uall[c, i, :, part] = uall[c, i, :, part] + gap if it > 0 else gap
                    zall[c, i, :, part] = fresh
            return primal, dual

        return repeat(bands, expand, sums)

    def deliver(c, marks):
        block = jnp.zeros(tile, f32)
        for n, distance in enumerate(sorted({1, bands // 2})):
            source = gains[ITERS - 1, c, behind(distance)]
            for turn in range(subs):
                moved = pltpu.roll(source, turn * 2 * group, 0) if turn else source
                block = block + marks[n][turn] * moved
        for s in range(subs):
            for k in range(group):
                base = 2 * (s * group + k)
                delivered[s, c * group + k] = block[base : base + 2]

    first, after = {}, {}
    for c in range(chunks):
        for j in range(pairs):
            for copy in load(c, j):
                copy.wait()
        if c == 1:
            pl.semaphore_wait(barrier, bands - 1 + dirs - 1)
            for distance in range(1, bands):
                meta_copy(me, distance).start()
        steps = [build(c, first)]
        if c > 0:
            steps.insert(0, sweeps(0, c - 1, first[c - 1], after))
        together(*steps)
        if c > 0:
            send(0, c - 1, after[c - 1])
    for distance in range(1, bands):
        meta_copy(behind(distance), distance).wait_recv()
    together(sweeps(0, chunks - 1, first[chunks - 1], after))
    send(0, chunks - 1, after[chunks - 1])
    weight_sum = solve()

    zero = jnp.zeros((rows, LANES), f32)
    totals = [(zero, zero) for _ in range(ITERS)]
    pace = 2 if chunks % 2 == 0 else 1
    for base in range(0, chunks, pace):
        here = range(base, base + pace)
        for c in here:
            arrive(0, c)
            totals[0] = consensus(0, c, totals[0])
        together(*(sweeps(1, c, gains[0, c, me], after) for c in here))
        for c in here:
            send(1, c, after[c])

    marks = []
    lane_rows = (rows, LANES)
    for distance in sorted({1, bands // 2}):
        source = behind(distance)
        by_turn = []
        for turn in range(subs):
            mark = jnp.zeros(tile, f32)
            for s in range(subs):
                wanted = (me * subs + s).astype(f32)
                r = (s - turn) % subs
                here = (meta[source, r : r + 1, 0:LANES] == wanted).astype(f32)
                mark = jnp.where(sub_row == s, spread(here[:, 0:1], tile), mark)
            by_turn.append(mark)
        marks.append(by_turn)
    for c in range(chunks):
        arrive(1, c)
        totals[1] = consensus(1, c, totals[1])
        deliver(c, marks)

    norm_tile = jnp.zeros((TILE, LANES), f32)
    for it in range(ITERS):
        for j in range(2):
            norm_tile = jnp.where(
                row_of(norm_tile.shape) == 2 * it + j,
                jnp.sum(totals[it][j], axis=0, keepdims=True),
                norm_tile,
            )
    norm_all[my_dir] = norm_tile
    for distance in range(1, dirs):
        norm_copy(my_dir, distance).start()
    for distance in range(1, dirs):
        norm_copy(lax.rem(my_dir + dirs - distance, dirs), distance).wait_recv()
    sum_tile = norm_all[0]
    for i in range(1, dirs):
        sum_tile = sum_tile + norm_all[i]
    sums = jnp.sum(sum_tile, axis=1, keepdims=True)
    final = jnp.sqrt(sums / (count * dirs * 2.0 * stations * weight_sum))
    for it in range(ITERS):
        for j in range(2):
            norms[it : it + 1, j : j + 1] = final[2 * it + j : 2 * it + j + 1]

    for distance in range(1, dirs):
        norm_copy(my_dir, distance).wait_send()
    for distance in range(1, bands):
        meta_copy(me, distance).wait_send()
        for it in range(ITERS):
            for c in range(chunks):
                gain_copy(it, c, me, distance).wait_send()


def per_device(bands, dirs, visibilities, sky_model, rfi_flags, destination):
    subs, count, _, stations, _ = visibilities.shape
    total = bands * subs
    width = -(-total // LANES) * LANES
    meta_rows = -(-(subs + 1) // 8) * 8
    group = max(1, TILE // (2 * subs))
    chunks = count // group
    pairs = subs * group
    rows = 2 * pairs
    vmem = pl.BlockSpec(memory_space=pltpu.VMEM)
    hbm = pl.BlockSpec(memory_space=pl.ANY)
    sem = pltpu.SemaphoreType.DMA
    delivered, coefficients, norms = pl.pallas_call(
        functools.partial(kernel, bands, dirs, group),
        out_shape=(
            pltpu.VMEM((subs, count, 2, stations), f32),
            pltpu.VMEM((TERMS, count, 2, stations), f32),
            pltpu.VMEM((ITERS, 2), f32),
        ),
        in_specs=[hbm, hbm, vmem, pl.BlockSpec(memory_space=pltpu.SMEM)],
        out_specs=(vmem, vmem, vmem),
        scratch_shapes=[
            pltpu.VMEM((subs * count, 2, stations, stations), bf16),
            pltpu.VMEM((subs * count, 2, stations, stations), bf16),
            pltpu.VMEM((chunks, 2 * pairs * stations, stations), bf16),
            pltpu.VMEM((chunks, pairs * stations, stations), bf16),
            pltpu.VMEM((chunks, 2 * pairs * stations, stations), bf16),
            pltpu.VMEM((chunks, pairs * stations, stations), bf16),
            pltpu.VMEM((pairs, 4, stations, stations), f32),
            pltpu.VMEM((subs, stations, stations), f32),
            pltpu.VMEM((rows, stations), f32),
            pltpu.VMEM((bands, meta_rows, width), f32),
            pltpu.VMEM((ITERS, chunks, bands, rows, stations), f32),
            pltpu.VMEM((chunks, bands, rows, stations), f32),
            pltpu.VMEM((chunks, bands, rows, stations), f32),
            pltpu.VMEM((chunks, 2, rows, stations), f32),
            pltpu.VMEM((total, ROWS, LANES), f32),
            pltpu.VMEM((total, ROWS, LANES), f32),
            pltpu.VMEM((bands, TERMS, rows, LANES), f32),
            pltpu.VMEM((bands, TERMS + 1, rows, LANES), f32),
            pltpu.VMEM((dirs, TILE, LANES), f32),
            sem((subs * count,)),
            sem((subs * count,)),
            sem((bands,)),
            sem((bands,)),
            sem((ITERS, chunks, bands)),
            sem((ITERS, chunks, bands)),
            sem((dirs,)),
            sem((dirs,)),
        ],
        compiler_params=pltpu.CompilerParams(
            collective_id=0, has_side_effects=True, vmem_limit_bytes=56 * 1024 * 1024
        ),
    )(visibilities, sky_model, rfi_flags, destination)
    return delivered, coefficients, norms


def solution(mesh):
    return jax.shard_map(
        functools.partial(per_device, mesh.shape["band"], mesh.shape["dir"]),
        mesh=mesh,
        in_specs=(
            P("band", "dir", None, None, None),
            P("band", "dir", None, None, None),
            P("band", None, None),
            P("band"),
        ),
        out_specs=(P("band", "dir", None, None), P(None, "dir", None, None), P()),
        check_vma=False,
    )
```

```python
import functools

import jax
import jax.numpy as jnp
from jax import lax
from jax.experimental import pallas as pl
from jax.experimental.pallas import tpu as pltpu
from jax.sharding import PartitionSpec as P

BLOCK = 32
DEGREE = 8
SWEEPS = 4
ITERS = 2
TERMS = DEGREE + 1
ROWS = 16
LANES = 128
TILE = 8
PLAN = (("exact", "lead", "both", "held"), ("held", "held", "both", "held"))

penalty_share = 0.4
f32 = jnp.float32
bf16 = jnp.bfloat16
MESH = pl.DeviceIdType.MESH


def row_of(shape, axis=0):
    return lax.broadcasted_iota(jnp.int32, shape, axis)


def spread(value, shape):
    return jnp.broadcast_to(value, shape)


def repeat(count, body, carry):
    if count <= 8:
        for i in range(count):
            carry = body(i, carry)
        return carry
    return lax.fori_loop(0, count, body, carry)


def kernel(
    bands,
    dirs,
    group,
    vis_hbm,
    sky_hbm,
    flags_hbm,
    dest_hbm,
    delivered,
    coef,
    norms,
    flags,
    dest,
    vis,
    sky,
    lead_num,
    lead_den,
    rest_num,
    rest_den,
    turned,
    keep,
    wpen,
    meta,
    gains,
    zall,
    uall,
    held,
    solve_rows,
    cheb_rows,
    solve_tiles,
    cheb_tiles,
    norm_all,
    small_sem,
    load_sem,
    meta_send,
    meta_recv,
    gain_send,
    gain_recv,
    norm_send,
    norm_recv,
):
    subs, count, _, stations, _ = vis_hbm.shape
    blocks = flags.shape[-1]
    total = bands * subs
    width = meta.shape[-1]
    chunks = count // group
    pairs = subs * group
    rows = 2 * pairs
    me = lax.axis_index("band")
    my_dir = lax.axis_index("dir")
    tile = (rows, stations)

    def across(distance):
        peer, bit = me, 1
        while bit <= distance:
            if distance // bit % 2:
                peer = peer + bit - 2 * bit * lax.rem(me // bit, 2)
            bit *= 2
        return peer

    if bands & (bands - 1) == 0:
        peers = [across(distance) for distance in range(bands - 1, 0, -1)]
    else:
        peers = [lax.rem(me + distance, bands) for distance in range(1, bands)]

    def behind(distance):
        return lax.rem(me + bands - distance, bands)

    def load(c):
        part = pl.ds(c * group, group)
        return (
            pltpu.make_async_copy(vis_hbm.at[:, part], vis.at[c], load_sem.at[0, c]),
            pltpu.make_async_copy(sky_hbm.at[:, part], sky.at[c], load_sem.at[1, c]),
        )

    small = (
        pltpu.make_async_copy(flags_hbm, flags, small_sem.at[0]),
        pltpu.make_async_copy(dest_hbm, dest, small_sem.at[1]),
    )
    for copy in small:
        copy.start()
    for copy in load(0):
        copy.start()

    barrier = pltpu.get_barrier_semaphore()
    for peer in peers:
        pl.semaphore_signal(barrier, inc=1, device_id={"band": peer}, device_id_type=MESH)
    for distance in range(1, dirs):
        pl.semaphore_signal(
            barrier,
            inc=1,
            device_id={"dir": lax.rem(my_dir + distance, dirs)},
            device_id_type=MESH,
        )

    for copy in small:
        copy.wait()
    for copy in load(1) if chunks > 1 else ():
        copy.start()
    row = row_of(tile)
    odd = lax.rem(row, 2) == 1
    sub_row = row // (2 * group)

    lane_w = row_of((1, width), 1)
    weight_row = jnp.zeros((1, width), f32)
    penalty = jnp.zeros(tile, f32)
    dest_rows = []
    for s in range(subs):
        kept = (1 - flags[s]).astype(f32)
        weight = (1.0 + jnp.sum(kept, axis=(0, 1), keepdims=True)) / (1.0 + blocks * blocks)
        penalty = jnp.where(sub_row == s, spread(penalty_share * stations * weight, tile), penalty)
        weight_row = jnp.where(lane_w == me * subs + s, weight, weight_row)
        dest_rows.append(jnp.full((1, width), dest[s], jnp.int32).astype(f32))
        lane = row_of((1, stations), 1) // BLOCK
        for i in range(blocks):
            shape = (BLOCK, stations)
            across = jnp.zeros((1, stations), f32)
            for j in range(blocks):
                across = jnp.where(lane == j, kept[j : j + 1, i : i + 1], across)
            apart = row_of(shape) + i * BLOCK != row_of(shape, 1)
            keep[s, i * BLOCK : (i + 1) * BLOCK, :] = jnp.where(
                apart, spread(across, shape), 0.0
            )
    wpen[...] = penalty
    meta[me] = jnp.zeros(meta.shape[1:], f32)
    for s in range(subs):
        meta[me, s : s + 1, :] = dest_rows[s]
    meta[me, subs : subs + 1, :] = weight_row

    def meta_copy(slot, peer):
        return pltpu.make_async_remote_copy(
            src_ref=meta.at[slot],
            dst_ref=meta.at[slot],
            send_sem=meta_send,
            recv_sem=meta_recv,
            device_id={"band": peer},
            device_id_type=MESH,
        )

    def gain_copy(it, c, slot, peer):
        return pltpu.make_async_remote_copy(
            src_ref=gains.at[it, c, slot],
            dst_ref=gains.at[it, c, slot],
            send_sem=gain_send.at[it],
            recv_sem=gain_recv.at[it, c],
            device_id={"band": peer},
            device_id_type=MESH,
        )

    def norm_copy(slot, distance):
        return pltpu.make_async_remote_copy(
            src_ref=norm_all.at[slot],
            dst_ref=norm_all.at[slot],
            send_sem=norm_send,
            recv_sem=norm_recv,
            device_id={"dir": lax.rem(my_dir + distance, dirs)},
            device_id_type=MESH,
        )

    def all_of(ref, sem):
        return pltpu.make_async_copy(ref, ref, sem)

    square = (stations, stations)
    identity = (row_of(square) == row_of(square, 1)).astype(f32).astype(bf16)
    ones = jnp.where(odd, jnp.zeros(tile, f32), 1.0)

    def swapped(value):
        return jnp.where(odd, pltpu.roll(value, 1, 0), pltpu.roll(value, rows - 1, 0))

    pick_row = row_of((2 * rows, stations))
    pick_pair = lax.rem(pick_row, rows) // 2
    picks = [
        jnp.where(pick_pair == j, jnp.ones(pick_row.shape, f32), 0.0).astype(bf16)
        for j in range(pairs)
    ]

    def left_sides(gain):
        other = swapped(gain)
        sides = []
        for full in (gain, jnp.where(odd, other, -other), gain * gain + other * other):
            lead = full.astype(bf16).astype(f32)
            sides.append(jnp.concatenate([lead, full - lead], axis=0).astype(bf16))
        num, den = [], []
        for j in range(pairs):
            num += [sides[0] * picks[j], sides[1] * picks[j]]
            den.append(sides[2] * picks[j])
        return jnp.concatenate(num, axis=1), jnp.concatenate(den, axis=1)

    def times(left, right):
        out = lax.dot_general(
            left, right, (((1,), (0,)), ((), ())), preferred_element_type=f32
        )
        return out[:rows] + out[rows:]

    def solved(num, den, target):
        pen = wpen[...]
        return (num + pen * target) / (den + pen)

    def build(c, out):
        num = jnp.zeros(tile, f32)
        den = jnp.zeros(tile, f32)

        def turn(j):
            for part, source in enumerate((vis, sky)):
                for i in range(2):
                    turned[j, 2 * part + i] = lax.dot_general(
                        identity,
                        source[c, j // group, j % group, i],
                        (((1,), (1,)), ((), ())),
                        preferred_element_type=f32,
                    )

        def fill(j, num, den):
            s = j // group
            sums = [jnp.zeros((TILE, stations), f32) for _ in range(3)]
            for i in range(stations // BLOCK):
                part = slice(i * BLOCK, (i + 1) * BLOCK)
                baseline = keep[s, part, :]
                data_re = turned[j, 0, part, :]
                data_im = turned[j, 1, part, :]
                model_re = baseline * turned[j, 2, part, :]
                model_im = baseline * turned[j, 3, part, :]
                values = (
                    model_re * data_re + model_im * data_im,
                    model_re * data_im - model_im * data_re,
                    model_re * model_re + model_im * model_im,
                )
                for n, full in enumerate(values):
                    for r in range(0, BLOCK, TILE):
                        sums[n] = sums[n] + full[r : r + TILE]
                    lead = full.astype(bf16)
                    rest = (full - lead.astype(f32)).astype(bf16)
                    if n < 2:
                        base = (2 * j + n) * stations + i * BLOCK
                        lead_num[c, base : base + BLOCK, :] = lead
                        rest_num[c, base : base + BLOCK, :] = rest
                    else:
                        base = j * stations + i * BLOCK
                        lead_den[c, base : base + BLOCK, :] = lead
                        rest_den[c, base : base + BLOCK, :] = rest
            re, im, mag = (spread(jnp.sum(x, axis=0, keepdims=True), tile) for x in sums)
            num = jnp.where(row == 2 * j, re, jnp.where(row == 2 * j + 1, im, num))
            den = jnp.where(row // 2 == j, mag, den)
            return num, den

        for j in range(pairs):
            turn(j)
            num, den = fill(j, num, den)
            yield
        out[c] = solved(num, den, ones)

    def sweeps(it, c, gain, out):
        target = ones if it == 0 else zall[c, me] - uall[c, me]
        for index in range(SWEEPS):
            mode = PLAN[it][index]
            if mode == "exact":
                continue
            left_num, left_den = left_sides(gain)
            num = times(left_num, lead_num[c])
            den = times(left_den, lead_den[c])
            if mode == "both":
                low_num = times(left_num, rest_num[c])
                low_den = times(left_den, rest_den[c])
                held[c, 0] = low_num
                held[c, 1] = low_den
                num, den = num + low_num, den + low_den
            yield
            if mode == "held":
                num, den = num + held[c, 0], den + held[c, 1]
            updated = solved(num, den, target)
            gain = 0.5 * (updated + gain) if index % 2 == 1 else updated
        out[c] = gain

    def together(*steps):
        steps = list(steps)
        while steps:
            for step in list(steps):
                try:
                    next(step)
                except StopIteration:
                    steps.remove(step)

    def send(it, c, gain):
        gains[it, c, me] = gain
        for peer in peers:
            gain_copy(it, c, me, peer).start()

    def arrive(it, c):
        all_of(gains.at[it, c, pl.ds(0, bands - 1)], gain_recv.at[it, c]).wait()

    def solve(out):
        weights = meta[0, subs : subs + 1, :]
        for i in range(1, bands):
            weights = weights + meta[i, subs : subs + 1, :]
        index = row_of((1, width), 1).astype(f32)
        abscissa = (2.0 * index + 1.0) / total - 1.0
        terms = [jnp.ones_like(abscissa), abscissa]
        for degree in range(2, DEGREE + 1):
            terms.append(2.0 * abscissa * terms[-1] - terms[-2])
        shape = (ROWS, width)
        cheb = jnp.zeros(shape, f32)
        for c in range(TERMS):
            cheb = jnp.where(row_of(shape) == c, spread(terms[c], shape), cheb)
        right = cheb * weights
        gram = jnp.zeros((ROWS, LANES), f32)
        for c in range(TERMS):
            column = jnp.sum(right * terms[c], axis=1, keepdims=True)
            gram = jnp.where(row_of(gram.shape, 1) == c, column, gram)
        yield
        for c in range(TERMS):
            pivot = gram[c : c + 1, c : c + 1]
            gram_row = gram[c : c + 1, :] / pivot
            right_row = right[c : c + 1, :] / pivot
            column = gram[:, c : c + 1]
            gram = jnp.where(row_of(gram.shape) == c, gram_row, gram - column * gram_row)
            right = jnp.where(row_of(shape) == c, right_row, right - column * right_row)
        yield
        cheb = jnp.where(row_of(shape) == ROWS - 1, spread(weights, shape), cheb)
        for f in range(total):
            solve_rows[f] = spread(right[:, f : f + 1], (ROWS, LANES))
            cheb_rows[f] = spread(cheb[:, f : f + 1], (ROWS, LANES))

        half = (rows, LANES)
        sub = row_of(half) // (2 * group)

        def lay(i, carry):
            for source, tiles, used in (
                (solve_rows, solve_tiles, range(TERMS)),
                (cheb_rows, cheb_tiles, [*range(TERMS), ROWS - 1]),
            ):
                for n, c in enumerate(used):
                    value = spread(source[i * subs, c : c + 1, :], half)
                    for s in range(1, subs):
                        more = spread(source[i * subs + s, c : c + 1, :], half)
                        value = jnp.where(sub == s, more, value)
                    tiles[i, n] = value
            return carry

        repeat(bands, lay, 0)
        out["weights"] = jnp.sum(weights, axis=1, keepdims=True)

    def consensus(it, c, sums):
        parts = [slice(at, at + LANES) for at in range(0, stations, LANES)]
        zero = jnp.zeros((rows, LANES), f32)
        lanes = len(parts)

        def project(i, acc):
            values = []
            for part in parts:
                value = gains[it, c, i, :, part]
                if it > 0:
                    value = value + uall[c, i, :, part]
                values.append(value)
            acc = list(acc)
            for n in range(TERMS):
                scale = solve_tiles[i, n]
                for h in range(lanes):
                    acc[n * lanes + h] = acc[n * lanes + h] + scale * values[h]
            return tuple(acc)

        acc = repeat(bands, project, (zero,) * (TERMS * lanes))
        coefs = []
        for one in acc:
            value = one
            for s in range(1, subs):
                value = value + pltpu.roll(one, s * 2 * group, 0)
            coefs.append(value)
        if it == ITERS - 1:
            for n in range(TERMS):
                for h, part in enumerate(parts):
                    for k in range(group):
                        coef[n, c * group + k, :, part] = coefs[n * lanes + h][2 * k : 2 * k + 2]
        unit = jnp.where(lax.rem(row_of(zero.shape), 2) == 1, zero, 1.0)

        def expand(i, sums):
            primal, dual = sums
            scales = [cheb_tiles[i, n] for n in range(TERMS + 1)]
            for h, part in enumerate(parts):
                fresh = scales[0] * coefs[h]
                for n in range(1, TERMS):
                    fresh = fresh + scales[n] * coefs[n * lanes + h]
                gap = gains[it, c, i, :, part] - fresh
                moved = fresh - (zall[c, i, :, part] if it > 0 else unit)
                primal = primal + scales[TERMS] * (gap * gap)
                dual = dual + scales[TERMS] * (moved * moved)
                if it < ITERS - 1:
                    uall[c, i, :, part] = uall[c, i, :, part] + gap if it > 0 else gap
                    zall[c, i, :, part] = fresh
            return primal, dual

        return repeat(bands, expand, sums)

    def deliver(c, marks):
        block = jnp.zeros(tile, f32)
        for n, distance in enumerate(sorted({1, bands // 2})):
            source = gains[ITERS - 1, c, behind(distance)]
            for turn in range(subs):
                moved = pltpu.roll(source, turn * 2 * group, 0) if turn else source
                block = block + marks[n][turn] * moved
        for s in range(subs):
            for k in range(group):
                base = 2 * (s * group + k)
                delivered[s, c * group + k] = block[base : base + 2]

    first, after = {}, {}
    for c in range(chunks):
        for copy in load(c):
            copy.wait()
        for n in range(max(2, c + 2), chunks if c == 0 else 0):
            for copy in load(n):
                copy.start()
        if c == 1:
            pl.semaphore_wait(barrier, bands - 1 + dirs - 1)
            for peer in peers:
                meta_copy(me, peer).start()
        steps = [build(c, first)]
        if c > 0:
            steps.insert(0, sweeps(0, c - 1, first[c - 1], after))
        together(*steps)
        if c > 0:
            send(0, c - 1, after[c - 1])
    all_of(meta.at[pl.ds(0, bands - 1)], meta_recv).wait()
    together(solve(after), sweeps(0, chunks - 1, first[chunks - 1], after))
    send(0, chunks - 1, after[chunks - 1])
    weight_sum = after["weights"]

    zero = jnp.zeros((rows, LANES), f32)
    totals = [(zero, zero) for _ in range(ITERS)]
    pace = 2 if chunks % 2 == 0 else 1
    for base in range(0, chunks, pace):
        here = range(base, base + pace)
        for c in here:
            arrive(0, c)
            totals[0] = consensus(0, c, totals[0])
        together(*(sweeps(1, c, gains[0, c, me], after) for c in here))
        for c in here:
            send(1, c, after[c])

    marks = []
    lane_rows = (rows, LANES)
    for distance in sorted({1, bands // 2}):
        source = behind(distance)
        by_turn = []
        for turn in range(subs):
            mark = jnp.zeros(tile, f32)
            for s in range(subs):
                wanted = (me * subs + s).astype(f32)
                r = (s - turn) % subs
                here = (meta[source, r : r + 1, 0:LANES] == wanted).astype(f32)
                mark = jnp.where(sub_row == s, spread(here[:, 0:1], tile), mark)
            by_turn.append(mark)
        marks.append(by_turn)
    for c in range(chunks):
        arrive(1, c)
        totals[1] = consensus(1, c, totals[1])
        deliver(c, marks)

    norm_tile = jnp.zeros((TILE, LANES), f32)
    for it in range(ITERS):
        for j in range(2):
            norm_tile = jnp.where(
                row_of(norm_tile.shape) == 2 * it + j,
                jnp.sum(totals[it][j], axis=0, keepdims=True),
                norm_tile,
            )
    norm_all[my_dir] = norm_tile
    for distance in range(1, dirs):
        norm_copy(my_dir, distance).start()
    all_of(norm_all.at[pl.ds(0, dirs - 1)], norm_recv).wait()
    sum_tile = norm_all[0]
    for i in range(1, dirs):
        sum_tile = sum_tile + norm_all[i]
    sums = jnp.sum(sum_tile, axis=1, keepdims=True)
    final = jnp.sqrt(sums / (count * dirs * 2.0 * stations * weight_sum))
    for it in range(ITERS):
        for j in range(2):
            norms[it : it + 1, j : j + 1] = final[2 * it + j : 2 * it + j + 1]

    all_of(norm_all.at[pl.ds(0, dirs - 1)], norm_send).wait()
    all_of(meta.at[pl.ds(0, bands - 1)], meta_send).wait()
    for it in range(ITERS):
        all_of(gains.at[it, :, pl.ds(0, bands - 1)], gain_send.at[it]).wait()


def put_out(*refs):
    count = len(refs) // 2
    sems = refs[-1]
    copies = [
        pltpu.make_async_copy(refs[i], refs[count + i], sems.at[i]) for i in range(count)
    ]
    for copy in copies:
        copy.start()
    for copy in copies:
        copy.wait()


def per_device(bands, dirs, visibilities, sky_model, rfi_flags, destination):
    subs, count, _, stations, _ = visibilities.shape
    total = bands * subs
    width = -(-total // LANES) * LANES
    meta_rows = -(-(subs + 1) // 8) * 8
    group = max(1, TILE // (2 * subs))
    chunks = count // group
    pairs = subs * group
    rows = 2 * pairs
    vmem = pl.BlockSpec(memory_space=pltpu.VMEM)
    hbm = pl.BlockSpec(memory_space=pl.ANY)
    sem = pltpu.SemaphoreType.DMA
    delivered, coefficients, norms = pl.pallas_call(
        functools.partial(kernel, bands, dirs, group),
        out_shape=(
            pltpu.VMEM((subs, count, 2, stations), f32),
            pltpu.VMEM((TERMS, count, 2, stations), f32),
            pltpu.VMEM((ITERS, 2), f32),
        ),
        in_specs=[hbm, hbm, hbm, hbm],
        out_specs=(vmem, vmem, vmem),
        scratch_shapes=[
            pltpu.VMEM(rfi_flags.shape, jnp.int32),
            pltpu.SMEM(destination.shape, jnp.int32),
            pltpu.VMEM((chunks, subs, group, 2, stations, stations), bf16),
            pltpu.VMEM((chunks, subs, group, 2, stations, stations), bf16),
            pltpu.VMEM((chunks, 2 * pairs * stations, stations), bf16),
            pltpu.VMEM((chunks, pairs * stations, stations), bf16),
            pltpu.VMEM((chunks, 2 * pairs * stations, stations), bf16),
            pltpu.VMEM((chunks, pairs * stations, stations), bf16),
            pltpu.VMEM((pairs, 4, stations, stations), f32),
            pltpu.VMEM((subs, stations, stations), f32),
            pltpu.VMEM((rows, stations), f32),
            pltpu.VMEM((bands, meta_rows, width), f32),
            pltpu.VMEM((ITERS, chunks, bands, rows, stations), f32),
            pltpu.VMEM((chunks, bands, rows, stations), f32),
            pltpu.VMEM((chunks, bands, rows, stations), f32),
            pltpu.VMEM((chunks, 2, rows, stations), f32),
            pltpu.VMEM((total, ROWS, LANES), f32),
            pltpu.VMEM((total, ROWS, LANES), f32),
            pltpu.VMEM((bands, TERMS, rows, LANES), f32),
            pltpu.VMEM((bands, TERMS + 1, rows, LANES), f32),
            pltpu.VMEM((dirs, TILE, LANES), f32),
            sem((2,)),
            sem((2, chunks)),
            sem(()),
            sem(()),
            sem((ITERS,)),
            sem((ITERS, chunks)),
            sem(()),
            sem(()),
        ],
        compiler_params=pltpu.CompilerParams(
            collective_id=0, has_side_effects=True, vmem_limit_bytes=56 * 1024 * 1024
        ),
    )(visibilities, sky_model, rfi_flags, destination)
    found = tuple(
        pltpu.with_memory_space_constraint(x, pltpu.MemorySpace.VMEM)
        for x in (delivered, coefficients, norms)
    )
    return pl.pallas_call(
        put_out,
        out_shape=tuple(jax.ShapeDtypeStruct(x.shape, x.dtype) for x in found),
        in_specs=[vmem] * len(found),
        out_specs=tuple([hbm] * len(found)),
        scratch_shapes=[sem((len(found),))],
    )(*found)


def solution(mesh):
    return jax.shard_map(
        functools.partial(per_device, mesh.shape["band"], mesh.shape["dir"]),
        mesh=mesh,
        in_specs=(
            P("band", "dir", None, None, None),
            P("band", "dir", None, None, None),
            P("band", None, None),
            P("band"),
        ),
        out_specs=(P("band", "dir", None, None), P(None, "dir", None, None), P()),
        check_vma=False,
    )
```

```python
import functools

import jax
import jax.numpy as jnp
from jax import lax
from jax.experimental import pallas as pl
from jax.experimental.pallas import tpu as pltpu
from jax.sharding import PartitionSpec as P

BLOCK = 32
DEGREE = 8
SWEEPS = 4
ITERS = 2
TERMS = DEGREE + 1
ROWS = 16
LANES = 128
TILE = 8
PLAN = (("exact", "lead", "both", "held"), ("held", "held", "both", "held"))

XLU = (2, 3)
WAIT_STEPS = 5
SPLIT = 2

penalty_share = 0.4
f32 = jnp.float32
bf16 = jnp.bfloat16
MESH = pl.DeviceIdType.MESH


def row_of(shape, axis=0):
    return lax.broadcasted_iota(jnp.int32, shape, axis)


def spread(value, shape):
    return jnp.broadcast_to(value, shape)


def repeat(count, body, carry):
    if count <= 8:
        for i in range(count):
            carry = body(i, carry)
        return carry
    return lax.fori_loop(0, count, body, carry)


def kernel(
    bands,
    dirs,
    group,
    vis_hbm,
    sky_hbm,
    flags_hbm,
    dest_hbm,
    delivered,
    coef,
    norms,
    flags,
    dest,
    vis,
    sky,
    lead_num,
    lead_den,
    rest_num,
    rest_den,
    turned,
    turned_low,
    keep,
    wpen,
    meta,
    gains,
    zall,
    uall,
    held,
    solve_rows,
    cheb_rows,
    solve_tiles,
    cheb_tiles,
    norm_all,
    small_sem,
    load_sem,
    meta_send,
    meta_recv,
    gain_send,
    gain_recv,
    norm_send,
    norm_recv,
):
    subs, count, _, stations, _ = vis_hbm.shape
    blocks = flags.shape[-1]
    total = bands * subs
    width = meta.shape[-1]
    chunks = count // group
    pairs = subs * group
    rows = 2 * pairs
    me = lax.axis_index("band")
    my_dir = lax.axis_index("dir")
    tile = (rows, stations)

    def across(distance):
        peer, bit = me, 1
        while bit <= distance:
            if distance // bit % 2:
                peer = peer + bit - 2 * bit * lax.rem(me // bit, 2)
            bit *= 2
        return peer

    if bands & (bands - 1) == 0:
        peers = [across(distance) for distance in range(bands - 1, 0, -1)]
    else:
        peers = [lax.rem(me + distance, bands) for distance in range(1, bands)]

    def behind(distance):
        return lax.rem(me + bands - distance, bands)

    def load(c):
        part = pl.ds(c * group, group)
        return (
            pltpu.make_async_copy(vis_hbm.at[:, part], vis.at[c], load_sem.at[0, c]),
            pltpu.make_async_copy(sky_hbm.at[:, part], sky.at[c], load_sem.at[1, c]),
        )

    small = (
        pltpu.make_async_copy(flags_hbm, flags, small_sem.at[0]),
        pltpu.make_async_copy(dest_hbm, dest, small_sem.at[1]),
    )
    for copy in small:
        copy.start()
    for copy in load(0):
        copy.start()

    barrier = pltpu.get_barrier_semaphore()
    for peer in peers:
        pl.semaphore_signal(barrier, inc=1, device_id={"band": peer}, device_id_type=MESH)
    for distance in range(1, dirs):
        pl.semaphore_signal(
            barrier,
            inc=1,
            device_id={"dir": lax.rem(my_dir + distance, dirs)},
            device_id_type=MESH,
        )

    for copy in small:
        copy.wait()
    for c in range(1, min(3, chunks)):
        for copy in load(c):
            copy.start()
    row = row_of(tile)
    odd = lax.rem(row, 2) == 1
    sub_row = row // (2 * group)

    lane_w = row_of((1, width), 1)
    weight_row = jnp.zeros((1, width), f32)
    penalty = jnp.zeros(tile, f32)
    dest_rows = []
    for s in range(subs):
        kept = (1 - flags[s]).astype(f32)
        weight = (1.0 + jnp.sum(kept, axis=(0, 1), keepdims=True)) / (1.0 + blocks * blocks)
        penalty = jnp.where(sub_row == s, spread(penalty_share * stations * weight, tile), penalty)
        weight_row = jnp.where(lane_w == me * subs + s, weight, weight_row)
        dest_rows.append(jnp.full((1, width), dest[s], jnp.int32).astype(f32))
        lane = row_of((1, stations), 1) // BLOCK
        for i in range(blocks):
            shape = (BLOCK, stations)
            line = jnp.zeros((1, stations), f32)
            for j in range(blocks):
                line = jnp.where(lane == j, kept[i : i + 1, j : j + 1], line)
            apart = row_of(shape) + i * BLOCK != row_of(shape, 1)
            keep[s, i * BLOCK : (i + 1) * BLOCK, :] = jnp.where(
                apart, spread(line, shape), 0.0
            ).astype(bf16)
    wpen[...] = penalty
    meta[me] = jnp.zeros(meta.shape[1:], f32)
    for s in range(subs):
        meta[me, s : s + 1, :] = dest_rows[s]
    meta[me, subs : subs + 1, :] = weight_row

    def meta_copy(slot, peer):
        return pltpu.make_async_remote_copy(
            src_ref=meta.at[slot],
            dst_ref=meta.at[slot],
            send_sem=meta_send,
            recv_sem=meta_recv,
            device_id={"band": peer},
            device_id_type=MESH,
        )

    def gain_copy(it, c, slot, peer):
        return pltpu.make_async_remote_copy(
            src_ref=gains.at[it, c, slot],
            dst_ref=gains.at[it, c, slot],
            send_sem=gain_send.at[it],
            recv_sem=gain_recv.at[it, c],
            device_id={"band": peer},
            device_id_type=MESH,
        )

    def norm_copy(slot, distance):
        return pltpu.make_async_remote_copy(
            src_ref=norm_all.at[slot],
            dst_ref=norm_all.at[slot],
            send_sem=norm_send,
            recv_sem=norm_recv,
            device_id={"dir": lax.rem(my_dir + distance, dirs)},
            device_id_type=MESH,
        )

    def all_of(ref, sem):
        return pltpu.make_async_copy(ref, ref, sem)

    square = (stations, stations)
    identity = (row_of(square) == row_of(square, 1)).astype(f32).astype(bf16)
    ones = jnp.where(odd, jnp.zeros(tile, f32), 1.0)

    def swapped(value):
        return jnp.where(odd, pltpu.roll(value, 1, 0), pltpu.roll(value, rows - 1, 0))

    pick_row = row_of((2 * rows, stations))
    pick_pair = lax.rem(pick_row, rows) // 2
    picks = [
        jnp.where(pick_pair == j, jnp.ones(pick_row.shape, f32), 0.0).astype(bf16)
        for j in range(pairs)
    ]

    def left_sides(gain):
        other = swapped(gain)
        sides = []
        for full in (gain, jnp.where(odd, other, -other), gain * gain + other * other):
            lead = full.astype(bf16).astype(f32)
            sides.append(jnp.concatenate([lead, full - lead], axis=0).astype(bf16))
        num, den = [], []
        for j in range(pairs):
            num += [sides[0] * picks[j], sides[1] * picks[j]]
            den.append(sides[2] * picks[j])
        return jnp.concatenate(num, axis=1), jnp.concatenate(den, axis=1)

    def times(left, right):
        out = lax.dot_general(
            left, right, (((1,), (0,)), ((), ())), preferred_element_type=f32
        )
        return out[:rows] + out[rows:]

    def solved(num, den, target):
        pen = wpen[...]
        return (num + pen * target) / (den + pen)

    def turn(c, j):
        s, k = j // group, j % group
        for n in range(4):
            value = vis[c, s, k, n] if n < 2 else sky[c, s, k, n - 2] * keep[s]
            if n in XLU:
                turned_low[j, n] = value.T
            else:
                turned[j, n] = lax.dot_general(
                    identity, value, (((1,), (1,)), ((), ())), preferred_element_type=f32
                )

    def build(c, out):
        num = jnp.zeros(tile, f32)
        den = jnp.zeros(tile, f32)
        if c < 3:
            turn(c, 0)
        for j in range(pairs):
            sums = [jnp.zeros((TILE, stations), f32) for _ in range(3)]
            for i in range(stations // BLOCK):
                part = slice(i * BLOCK, (i + 1) * BLOCK)
                data_re, data_im, model_re, model_im = (
                    turned_low[j, n, part, :].astype(f32) if n in XLU else turned[j, n, part, :]
                    for n in range(4)
                )
                values = (
                    model_re * data_re + model_im * data_im,
                    model_re * data_im - model_im * data_re,
                    model_re * model_re + model_im * model_im,
                )
                for n, full in enumerate(values):
                    for r in range(0, BLOCK, TILE):
                        sums[n] = sums[n] + full[r : r + TILE]
                    lead = full.astype(bf16)
                    rest = (full - lead.astype(f32)).astype(bf16)
                    if n < 2:
                        base = (2 * j + n) * stations + i * BLOCK
                        lead_num[c, base : base + BLOCK, :] = lead
                        rest_num[c, base : base + BLOCK, :] = rest
                    else:
                        base = j * stations + i * BLOCK
                        lead_den[c, base : base + BLOCK, :] = lead
                        rest_den[c, base : base + BLOCK, :] = rest
                if i == 0:
                    if j + 1 < pairs:
                        turn(c, j + 1)
                    elif 1 < c < chunks - 1:
                        turn(c + 1, 0)
                yield
            re, im, mag = (spread(jnp.sum(x, axis=0, keepdims=True), tile) for x in sums)
            num = jnp.where(row == 2 * j, re, jnp.where(row == 2 * j + 1, im, num))
            den = jnp.where(row // 2 == j, mag, den)
        out[c] = solved(num, den, ones)

    def sweeps(it, c, gain, out):
        target = ones if it == 0 else zall[c, me] - uall[c, me]
        for index in range(SWEEPS):
            mode = PLAN[it][index]
            if mode == "exact":
                continue
            left_num, left_den = left_sides(gain)
            step = stations * SPLIT
            products = {}
            for part, at_num, at_den in (
                ("lead", lead_num, lead_den),
                ("rest", rest_num, rest_den),
            ):
                if part == "rest" and mode != "both":
                    continue
                for j in range(0, pairs, SPLIT):
                    at = slice(j * stations, j * stations + step)
                    two = slice(2 * at.start, 2 * at.stop)
                    got = (
                        times(left_num[:, two], at_num[c, two, :]),
                        times(left_den[:, at], at_den[c, at, :]),
                    )
                    if part in products:
                        got = tuple(a + b for a, b in zip(products[part], got))
                    products[part] = got
                    yield False
            num, den = products["lead"]
            if mode == "both":
                low_num, low_den = products["rest"]
                held[c, 0] = low_num
                held[c, 1] = low_den
                num, den = num + low_num, den + low_den
            yield True
            if mode == "held":
                num, den = num + held[c, 0], den + held[c, 1]
            updated = solved(num, den, target)
            gain = 0.5 * (updated + gain) if index % 2 == 1 else updated
        out[c] = gain

    def coarse(steps):
        for ended in steps:
            if ended:
                yield

    def together(*steps):
        steps = list(steps)
        while steps:
            for step in list(steps):
                try:
                    next(step)
                except StopIteration:
                    steps.remove(step)

    def weave(main, side):
        for ended in main:
            for _ in range(WAIT_STEPS if ended else SPLIT):
                next(side, None)
        for _ in side:
            pass

    def send(it, c, gain):
        gains[it, c, me] = gain
        for peer in peers:
            gain_copy(it, c, me, peer).start()

    def arrive(it, c):
        all_of(gains.at[it, c, pl.ds(0, bands - 1)], gain_recv.at[it, c]).wait()

    def solve(out):
        weights = meta[0, subs : subs + 1, :]
        for i in range(1, bands):
            weights = weights + meta[i, subs : subs + 1, :]
        index = row_of((1, width), 1).astype(f32)
        abscissa = (2.0 * index + 1.0) / total - 1.0
        terms = [jnp.ones_like(abscissa), abscissa]
        for degree in range(2, DEGREE + 1):
            terms.append(2.0 * abscissa * terms[-1] - terms[-2])
        shape = (ROWS, width)
        cheb = jnp.zeros(shape, f32)
        for c in range(TERMS):
            cheb = jnp.where(row_of(shape) == c, spread(terms[c], shape), cheb)
        right = cheb * weights
        gram = jnp.zeros((ROWS, LANES), f32)
        for c in range(TERMS):
            column = jnp.sum(right * terms[c], axis=1, keepdims=True)
            gram = jnp.where(row_of(gram.shape, 1) == c, column, gram)
        yield
        for c in range(TERMS):
            pivot = gram[c : c + 1, c : c + 1]
            gram_row = gram[c : c + 1, :] / pivot
            right_row = right[c : c + 1, :] / pivot
            column = gram[:, c : c + 1]
            gram = jnp.where(row_of(gram.shape) == c, gram_row, gram - column * gram_row)
            right = jnp.where(row_of(shape) == c, right_row, right - column * right_row)
        yield
        cheb = jnp.where(row_of(shape) == ROWS - 1, spread(weights, shape), cheb)
        for f in range(total):
            solve_rows[f] = spread(right[:, f : f + 1], (ROWS, LANES))
            cheb_rows[f] = spread(cheb[:, f : f + 1], (ROWS, LANES))

        half = (rows, LANES)
        sub = row_of(half) // (2 * group)

        def lay(i, carry):
            for source, tiles, used in (
                (solve_rows, solve_tiles, range(TERMS)),
                (cheb_rows, cheb_tiles, [*range(TERMS), ROWS - 1]),
            ):
                for n, c in enumerate(used):
                    value = spread(source[i * subs, c : c + 1, :], half)
                    for s in range(1, subs):
                        more = spread(source[i * subs + s, c : c + 1, :], half)
                        value = jnp.where(sub == s, more, value)
                    tiles[i, n] = value
            return carry

        repeat(bands, lay, 0)
        out["weights"] = jnp.sum(weights, axis=1, keepdims=True)

    def consensus(it, c, sums):
        parts = [slice(at, at + LANES) for at in range(0, stations, LANES)]
        zero = jnp.zeros((rows, LANES), f32)
        lanes = len(parts)

        def project(i, acc):
            values = []
            for part in parts:
                value = gains[it, c, i, :, part]
                if it > 0:
                    value = value + uall[c, i, :, part]
                values.append(value)
            acc = list(acc)
            for n in range(TERMS):
                scale = solve_tiles[i, n]
                for h in range(lanes):
                    acc[n * lanes + h] = acc[n * lanes + h] + scale * values[h]
            return tuple(acc)

        acc = repeat(bands, project, (zero,) * (TERMS * lanes))
        coefs = []
        for one in acc:
            value = one
            for s in range(1, subs):
                value = value + pltpu.roll(one, s * 2 * group, 0)
            coefs.append(value)
        if it == ITERS - 1:
            for n in range(TERMS):
                for h, part in enumerate(parts):
                    for k in range(group):
                        coef[n, c * group + k, :, part] = coefs[n * lanes + h][2 * k : 2 * k + 2]
        unit = jnp.where(lax.rem(row_of(zero.shape), 2) == 1, zero, 1.0)

        def expand(i, sums):
            primal, dual = sums
            scales = [cheb_tiles[i, n] for n in range(TERMS + 1)]
            for h, part in enumerate(parts):
                fresh = scales[0] * coefs[h]
                for n in range(1, TERMS):
                    fresh = fresh + scales[n] * coefs[n * lanes + h]
                gap = gains[it, c, i, :, part] - fresh
                moved = fresh - (zall[c, i, :, part] if it > 0 else unit)
                primal = primal + scales[TERMS] * (gap * gap)
                dual = dual + scales[TERMS] * (moved * moved)
                if it < ITERS - 1:
                    uall[c, i, :, part] = uall[c, i, :, part] + gap if it > 0 else gap
                    zall[c, i, :, part] = fresh
            return primal, dual

        return repeat(bands, expand, sums)

    def deliver(c, marks):
        block = jnp.zeros(tile, f32)
        for n, distance in enumerate(sorted({1, bands // 2})):
            source = gains[ITERS - 1, c, behind(distance)]
            for turn in range(subs):
                moved = pltpu.roll(source, turn * 2 * group, 0) if turn else source
                block = block + marks[n][turn] * moved
        for s in range(subs):
            for k in range(group):
                base = 2 * (s * group + k)
                delivered[s, c * group + k] = block[base : base + 2]

    first, after = {}, {}
    for c in range(chunks):
        if c < 3:
            for copy in load(c):
                copy.wait()
        for n in range(3, chunks if c == 0 else 0):
            for copy in load(n):
                copy.start()
        if 1 < c < chunks - 1:
            for copy in load(c + 1):
                copy.wait()
        if c == 1:
            pl.semaphore_wait(barrier, bands - 1 + dirs - 1)
            for peer in peers:
                meta_copy(me, peer).start()
        if c == 0:
            together(build(c, first))
        else:
            weave(sweeps(0, c - 1, first[c - 1], after), build(c, first))
        if c > 0:
            send(0, c - 1, after[c - 1])
    all_of(meta.at[pl.ds(0, bands - 1)], meta_recv).wait()
    together(solve(after), coarse(sweeps(0, chunks - 1, first[chunks - 1], after)))
    send(0, chunks - 1, after[chunks - 1])
    weight_sum = after["weights"]

    zero = jnp.zeros((rows, LANES), f32)
    totals = [(zero, zero) for _ in range(ITERS)]
    pace = 2 if chunks % 2 == 0 else 1
    for base in range(0, chunks, pace):
        here = range(base, base + pace)
        if pace == 2 and base + pace == chunks:
            runs = []
            for c in here:
                arrive(0, c)
                totals[0] = consensus(0, c, totals[0])
                runs.append(coarse(sweeps(1, c, gains[0, c, me], after)))
                if c == base:
                    next(runs[0])
                    next(runs[0])
            for _ in range(2):
                next(runs[0])
                next(runs[1])
            for c, run in zip(here, runs):
                for _ in run:
                    pass
                send(1, c, after[c])
            continue
        for c in here:
            arrive(0, c)
            totals[0] = consensus(0, c, totals[0])
        together(*(coarse(sweeps(1, c, gains[0, c, me], after)) for c in here))
        for c in here:
            send(1, c, after[c])

    marks = []
    lane_rows = (rows, LANES)
    for distance in sorted({1, bands // 2}):
        source = behind(distance)
        by_turn = []
        for turn in range(subs):
            mark = jnp.zeros(tile, f32)
            for s in range(subs):
                wanted = (me * subs + s).astype(f32)
                r = (s - turn) % subs
                here = (meta[source, r : r + 1, 0:LANES] == wanted).astype(f32)
                mark = jnp.where(sub_row == s, spread(here[:, 0:1], tile), mark)
            by_turn.append(mark)
        marks.append(by_turn)
    for c in range(chunks):
        arrive(1, c)
        totals[1] = consensus(1, c, totals[1])
        deliver(c, marks)

    norm_tile = jnp.zeros((TILE, LANES), f32)
    for it in range(ITERS):
        for j in range(2):
            norm_tile = jnp.where(
                row_of(norm_tile.shape) == 2 * it + j,
                jnp.sum(totals[it][j], axis=0, keepdims=True),
                norm_tile,
            )
    norm_all[my_dir] = norm_tile
    for distance in range(1, dirs):
        norm_copy(my_dir, distance).start()
    all_of(norm_all.at[pl.ds(0, dirs - 1)], norm_recv).wait()
    sum_tile = norm_all[0]
    for i in range(1, dirs):
        sum_tile = sum_tile + norm_all[i]
    sums = jnp.sum(sum_tile, axis=1, keepdims=True)
    final = jnp.sqrt(sums / (count * dirs * 2.0 * stations * weight_sum))
    for it in range(ITERS):
        for j in range(2):
            norms[it : it + 1, j : j + 1] = final[2 * it + j : 2 * it + j + 1]

    all_of(norm_all.at[pl.ds(0, dirs - 1)], norm_send).wait()
    all_of(meta.at[pl.ds(0, bands - 1)], meta_send).wait()
    for it in range(ITERS):
        all_of(gains.at[it, :, pl.ds(0, bands - 1)], gain_send.at[it]).wait()


def put_out(*refs):
    count = len(refs) // 2
    sems = refs[-1]
    copies = [
        pltpu.make_async_copy(refs[i], refs[count + i], sems.at[i]) for i in range(count)
    ]
    for copy in copies:
        copy.start()
    for copy in copies:
        copy.wait()


def per_device(bands, dirs, visibilities, sky_model, rfi_flags, destination):
    subs, count, _, stations, _ = visibilities.shape
    total = bands * subs
    width = -(-total // LANES) * LANES
    meta_rows = -(-(subs + 1) // 8) * 8
    group = max(1, TILE // (2 * subs))
    chunks = count // group
    pairs = subs * group
    rows = 2 * pairs
    vmem = pl.BlockSpec(memory_space=pltpu.VMEM)
    hbm = pl.BlockSpec(memory_space=pl.ANY)
    sem = pltpu.SemaphoreType.DMA
    delivered, coefficients, norms = pl.pallas_call(
        functools.partial(kernel, bands, dirs, group),
        out_shape=(
            pltpu.VMEM((subs, count, 2, stations), f32),
            pltpu.VMEM((TERMS, count, 2, stations), f32),
            pltpu.VMEM((ITERS, 2), f32),
        ),
        in_specs=[hbm, hbm, hbm, hbm],
        out_specs=(vmem, vmem, vmem),
        scratch_shapes=[
            pltpu.VMEM(rfi_flags.shape, jnp.int32),
            pltpu.SMEM(destination.shape, jnp.int32),
            pltpu.VMEM((chunks, subs, group, 2, stations, stations), bf16),
            pltpu.VMEM((chunks, subs, group, 2, stations, stations), bf16),
            pltpu.VMEM((chunks, 2 * pairs * stations, stations), bf16),
            pltpu.VMEM((chunks, pairs * stations, stations), bf16),
            pltpu.VMEM((chunks, 2 * pairs * stations, stations), bf16),
            pltpu.VMEM((chunks, pairs * stations, stations), bf16),
            pltpu.VMEM((pairs, 4, stations, stations), f32),
            pltpu.VMEM((pairs, 4, stations, stations), bf16),
            pltpu.VMEM((subs, stations, stations), bf16),
            pltpu.VMEM((rows, stations), f32),
            pltpu.VMEM((bands, meta_rows, width), f32),
            pltpu.VMEM((ITERS, chunks, bands, rows, stations), f32),
            pltpu.VMEM((chunks, bands, rows, stations), f32),
            pltpu.VMEM((chunks, bands, rows, stations), f32),
            pltpu.VMEM((chunks, 2, rows, stations), f32),
            pltpu.VMEM((total, ROWS, LANES), f32),
            pltpu.VMEM((total, ROWS, LANES), f32),
            pltpu.VMEM((bands, TERMS, rows, LANES), f32),
            pltpu.VMEM((bands, TERMS + 1, rows, LANES), f32),
            pltpu.VMEM((dirs, TILE, LANES), f32),
            sem((2,)),
            sem((2, chunks)),
            sem(()),
            sem(()),
            sem((ITERS,)),
            sem((ITERS, chunks)),
            sem(()),
            sem(()),
        ],
        compiler_params=pltpu.CompilerParams(
            collective_id=0, has_side_effects=True, vmem_limit_bytes=56 * 1024 * 1024
        ),
    )(visibilities, sky_model, rfi_flags, destination)
    found = tuple(
        pltpu.with_memory_space_constraint(x, pltpu.MemorySpace.VMEM)
        for x in (delivered, coefficients, norms)
    )
    return pl.pallas_call(
        put_out,
        out_shape=tuple(jax.ShapeDtypeStruct(x.shape, x.dtype) for x in found),
        in_specs=[vmem] * len(found),
        out_specs=tuple([hbm] * len(found)),
        scratch_shapes=[sem((len(found),))],
    )(*found)


def solution(mesh):
    return jax.shard_map(
        functools.partial(per_device, mesh.shape["band"], mesh.shape["dir"]),
        mesh=mesh,
        in_specs=(
            P("band", "dir", None, None, None),
            P("band", "dir", None, None, None),
            P("band", None, None),
            P("band"),
        ),
        out_specs=(P("band", "dir", None, None), P(None, "dir", None, None), P()),
        check_vma=False,
    )
```
